32 devices in a mesh: row: 4 (over z), col: 8 (over y, x, core).
Axes of the slice: x: 2, y: 2, z: 4, core: 2. Of those that a mesh axis runs over, the one named last changes fastest.
Arguments:
- tiles: bfloat16 [4, 8, 128, 128, 128], P('row', 'col'), may hold values from -6 to 6
- tile_row: int32 [4, 8, 128], P('row', 'col'), may hold values from 0 to 63, as said below
- tile_col: int32 [4, 8, 128], P('row', 'col'), may hold values from 0 to 31
- tile_count: int32 [4, 8], P('row', 'col'), may hold values from 16 to 128, as said below
- query_ids: int32 [128], replicated, may hold values from 0 to 32767
- damping: float32 [128], replicated, may hold values from 0.006629126 to 0.026516505
Outputs:
- scores: float32 [32768, 128], P(('row', 'col'))
The draws below stay inside these ranges and needn't reach their ends.
Inputs may be any that keep to these rules, and one draw needn't show every extreme that they name: `tile_count`: some device holds exactly 128 live slots; slots at or past the count hold arbitrary finite values and are ignored. `tile_row`: positions may repeat within a device; such tiles add. For every device and every col index o, the live slots name at most 4 distinct values among o * 8 to o * 8 + 7, and every device reaches 4 for some o. `query_ids`: ids may repeat.
All inputs are finite; a program needn't handle non-finite values.
Results may differ from the reference program's by a relative error of at most 0.003.
Values may be sent and summed in bfloat16 or wider, within the bound.
A program may use at most 128 MiB of HBM per device.

```python
import math
import jax
import jax.numpy as jnp
from jax import lax

TILE = 128
BPD = 8
TILES_DEV = 128
QUERIES = 128
TERMS = 4
TOUCH = 4
NBLK = 256
NODES = 32768
N_ROW = 4
N_COL = 8


def draw_tile_count(key, part):
    shifts = jax.random.randint(key, (N_ROW * N_COL,), 0, 4)
    counts = jnp.right_shift(jnp.full((N_ROW * N_COL,), TILES_DEV, jnp.int32), shifts.astype(jnp.int32))
    fullest = jax.random.randint(jax.random.fold_in(key, 7), (), 0, N_ROW * N_COL)
    counts = counts.at[fullest].set(TILES_DEV)
    return counts.reshape(N_ROW, N_COL).astype(jnp.int32)


def draw_tile_row(key, part):
    devs = N_ROW * N_COL
    owners = jax.random.randint(jax.random.fold_in(key, 11), (devs, TILES_DEV), 0, N_COL)
    starts = jax.random.randint(jax.random.fold_in(key, 12), (devs, N_COL), 0, BPD)
    offsets = jax.random.randint(jax.random.fold_in(key, 13), (devs, TILES_DEV), 0, TOUCH)
    favoured = jax.random.randint(jax.random.fold_in(key, 14), (devs,), 0, N_COL)
    slot = jnp.arange(TILES_DEV, dtype=jnp.int32)
    first = slot < TOUCH
    owners = jnp.where(first[None, :], favoured[:, None], owners)
    offsets = jnp.where(first[None, :], slot[None, :], offsets)
    chosen = jnp.take_along_axis(starts, owners, axis=1)
    local = (chosen + offsets) % BPD
    return (owners * BPD + local).reshape(N_ROW, N_COL, TILES_DEV).astype(jnp.int32)


def with_ends(array, stream_key, low, top_value):
    longest = array.shape.index(max(array.shape))
    spots = []
    for shift in (0, 1):
        where = [jax.random.randint(jax.random.fold_in(stream_key, axis), (), 0, length) for axis, length in enumerate(array.shape)]
        where[longest] = (where[longest] + shift) % array.shape[longest]
        spots.append(tuple(where))
    return array.at[spots[0]].set(low).at[spots[1]].set(top_value)


def levels(key, extent, pieces, least, largest):
    loudness, own = 1.0, jax.random.fold_in(key, 6)
    for dim, shards_of in pieces:
        steps = jnp.exp(jax.random.uniform(jax.random.fold_in(own, dim), (shards_of,), jnp.float32, least / len(pieces), largest / len(pieces)))
        loudness = loudness * jnp.repeat(steps, extent[dim] // shards_of).reshape([-1 if axis == dim else 1 for axis in range(len(extent))])
    return loudness


def normal_values(key, extent, scale, bound, cuts=(), kind=jnp.bfloat16):
    entries = scale * jax.random.normal(key, extent, jnp.float32)
    if cuts:
        entries = entries * levels(key, extent, cuts, -0.22, 0.18)
    return jnp.clip(entries, -bound, bound).astype(kind)


def setup_inputs(seed: int = 0) -> dict:
    keys = jax.random.split(jax.random.key(seed), 7)
    return {
        "tiles": normal_values(keys[0], (N_ROW, N_COL, TILES_DEV, TILE, TILE), 1.0, 6.0, ((0, 4), (1, 8))),
        "tile_row": draw_tile_row(jax.random.fold_in(keys[6], 71), 0),
        "tile_col": with_ends(jax.random.randint(keys[2], (N_ROW, N_COL, TILES_DEV), 0, BPD * N_ROW), jax.random.fold_in(keys[2], 1), 0, (BPD * N_ROW) - 1).astype(jnp.int32),
        "tile_count": draw_tile_count(jax.random.fold_in(keys[6], 71), 0),
        "query_ids": with_ends(jax.random.randint(keys[4], (QUERIES,), 0, NODES), jax.random.fold_in(keys[4], 1), 0, NODES - 1).astype(jnp.int32),
        "damping": jnp.clip(jnp.exp(jax.random.uniform(keys[5], (QUERIES,), jnp.float32, math.log(0.006629126), math.log(0.026516505))), 0.006629126, 0.026516505),
    }


def device_partial(tile_block, rows, cols, count, xcol):
    picked = xcol[cols]
    prod = jnp.einsum("tab,tbq->taq", tile_block.astype(jnp.float32), picked.astype(jnp.float32))
    live = (jnp.arange(tile_block.shape[0], dtype=jnp.int32) < count).astype(jnp.float32)
    prod = prod * live[:, None, None]
    return jax.ops.segment_sum(prod, rows, num_segments=BPD * N_COL)


def reference(tiles, tile_row, tile_col, tile_count, query_ids, damping):
    nodes = NBLK * TILE
    queries = query_ids.shape[0]
    node_ids = jnp.arange(nodes, dtype=jnp.int32)
    xvec = (node_ids[:, None] == query_ids[None, :]).astype(jnp.bfloat16)
    scores = jnp.zeros((nodes, queries), jnp.float32)
    coef = jnp.ones((queries,), jnp.float32)
    for step in range(TERMS):
        xgrid = xvec.reshape(N_ROW, N_COL, BPD, TILE, queries)

        def one_row(ridx):
            def add_col(cidx, total):
                xcol = lax.dynamic_index_in_dim(xgrid, cidx, 1, keepdims=False)
                xcol = xcol.reshape(N_ROW * BPD, TILE, queries)
                tblock = tiles[ridx, cidx]
                part = device_partial(tblock, tile_row[ridx, cidx], tile_col[ridx, cidx], tile_count[ridx, cidx], xcol)
                rounded = lax.optimization_barrier(part.astype(jnp.bfloat16))
                return total + rounded.astype(jnp.float32)

            start = jnp.zeros((BPD * N_COL, TILE, queries), jnp.float32)
            return lax.fori_loop(0, N_COL, add_col, start)

        ysum = lax.map(one_row, jnp.arange(N_ROW, dtype=jnp.int32))
        ysum = ysum.reshape(nodes, queries)
        scores = scores + coef[None, :] * ysum
        coef = coef * damping
        xvec = ysum.astype(jnp.bfloat16)
    return scores
```

```python
import functools

import jax
import jax.numpy as jnp
from jax import lax
from jax.experimental import pallas as pl
from jax.experimental.pallas import tpu as pltpu
from jax.sharding import PartitionSpec as P

BPD = 8
TERMS = 4
TOUCH = 4
GROUPS = 8
UNROLL = 64
CHUNKS = 8
LAG = 3
RELAY_LAG = 5
DIRECT = GROUPS
MESH = pl.DeviceIdType.MESH


def plan(rows, cols, count, n_col, me_col):
    slots = rows.shape[1]
    row_blocks = BPD * n_col
    square = (slots, slots)
    lane = lax.broadcasted_iota(jnp.int32, square, 1)
    sub = lax.broadcasted_iota(jnp.int32, square, 0)

    def across(row):
        return jnp.broadcast_to(row, square)

    def down(row):
        return jnp.transpose(jnp.broadcast_to(row, square))

    def total(mask, value=1):
        return jnp.sum(jnp.where(mask, value, 0), axis=0, keepdims=True)

    key = jnp.where(lane[:1] < count, rows, row_blocks)
    key_l, key_s = across(key), down(key)
    twin = (key_s == key_l) & (sub < lane)
    rank = total((key_s < key_l) | twin)
    again = jnp.minimum(total(twin), 1)
    packed = lane[:1] + slots * (again + 2 * cols)
    ordered = total(down(rank) == lane, down(packed))
    perm = lax.rem(ordered, slots)
    rest = lax.div(ordered, slots)
    cont = lax.rem(rest, 2)
    scol = lax.div(rest, 2)

    marked = jnp.minimum(total(key_s == lane), 1)
    marked = jnp.where(lane[:1] < row_blocks, marked, 0)
    last = total(key_s <= lane) - 1
    owner_l = lax.div(lane[:1], BPD)
    first = owner_l * BPD
    place = total((sub >= across(first)) & (sub < lane), down(marked))
    slot_of = jnp.where(marked > 0, owner_l * TOUCH + place, -1)
    ends = total(down(slot_of) == lane, down(last))
    pos = jnp.where(marked > 0, me_col * TOUCH + place, n_col * TOUCH)
    return perm, scol, cont, ends, pos


def katz_kernel(
    n_row, n_col,
    count_ref, rows_ref, cols_ref, qid_ref, damp_ref, tiles_hbm,
    out_ref,
    tiles, flip, run, send, got, xbuf, comp, total, coef, qcol, planbuf, posbuf, poszbuf, where, order, poz,
    tile_sem, pos_send, pos_recv, posz_send, posz_recv, local_sem, send_sem, recv_sem, xsend_sem, xrecv_sem, xpass_sem,
):
    me_r = lax.axis_index("row")
    me_c = lax.axis_index("col")
    slots, tile, _ = tiles.shape
    queries = qid_ref.shape[1]
    width = queries // GROUPS
    steps = TERMS * GROUPS
    moves = steps - GROUPS
    piece = slots // CHUNKS

    def load(i):
        part = pl.ds(i * piece, piece)
        return pltpu.make_async_copy(tiles_hbm.at[part], tiles.at[part], tile_sem.at[i])

    for i in range(CHUNKS):
        load(i).start()
    barrier = pltpu.get_barrier_semaphore()
    for d in range(1, n_col):
        pl.semaphore_signal(barrier, inc=1, device_id=(me_r, lax.rem(me_c + d, n_col)), device_id_type=MESH)
    for d in range(1, n_row):
        pl.semaphore_signal(barrier, inc=1, device_id=(lax.rem(me_r + d, n_row), me_c), device_id_type=MESH)

    perm, scol, cont, ends, pos = plan(rows_ref[...], cols_ref[...], count_ref[0, 0], n_col, me_c)
    planbuf[0:1, :] = perm
    planbuf[1:2, :] = scol
    planbuf[2:3, :] = cont
    planbuf[3:4, :] = ends
    planbuf[4:5, :] = pos
    posbuf[me_c] = pos
    spill = pltpu.make_async_copy(planbuf, order, local_sem)
    spill.start()

    lane = lax.broadcasted_iota(jnp.int32, (queries, tile), 1)
    ids = qid_ref[...]
    qid = jnp.transpose(jnp.broadcast_to(ids, (tile, queries))) - lane
    coef[...] = jnp.transpose(jnp.broadcast_to(damp_ref[...], (tile, queries)))
    home = lax.rem(lax.div(ids, BPD * tile), n_col)
    qcol[...] = jnp.transpose(jnp.broadcast_to(home, (tile, queries)))

    def first_x(j, carry):
        base = ((j // BPD * n_col + me_c) * BPD + lax.rem(j, BPD)) * tile
        hot = jnp.where(qid == base, 1.0, 0.0).astype(jnp.bfloat16)
        for h in range(GROUPS):
            xbuf[h][j] = hot[h * width:(h + 1) * width]
        return carry

    lax.fori_loop(0, n_row * BPD, first_x, 0)
    for t in range(GROUPS, steps):
        got[t][n_col * TOUCH] = jnp.zeros((width, tile), jnp.bfloat16)
    for i in range(CHUNKS):
        load(i).wait()

        def turn(s, carry):
            flip[s] = jnp.transpose(tiles[s])
            return carry

        lax.fori_loop(i * piece, (i + 1) * piece, turn, 0, unroll=8)
    spill.wait()

    def compute(t):
        def body(i, acc):
            for u in range(0, UNROLL, 2):
                p = i * UNROLL + u
                weights = jnp.concatenate([flip[order[0, p]], flip[order[0, p + 1]]], axis=1)
                both = jnp.concatenate([xbuf[t][order[1, p]], xbuf[t][order[1, p + 1]]], axis=0)
                prod = jnp.dot(both, weights, preferred_element_type=jnp.float32)
                acc = jnp.where(order[2, p] > 0, acc, 0.0) + prod[:width, :tile]
                run[p] = acc.astype(jnp.bfloat16)
                acc = jnp.where(order[2, p + 1] > 0, acc, 0.0) + prod[width:, tile:]
                run[p + 1] = acc.astype(jnp.bfloat16)
            return acc

        lax.fori_loop(0, slots // UNROLL, body, jnp.zeros((width, tile), jnp.float32))
        for s in range(n_col * TOUCH):
            send[t, s] = run[order[3, s]]
        for j in range(TOUCH):
            got[t][me_c * TOUCH + j] = run[order[3, me_c * TOUCH + j]]

    def part_copy(t, d):
        peer = lax.rem(me_c + d, n_col)
        return pltpu.make_async_remote_copy(
            src_ref=send.at[t, pl.ds(peer * TOUCH, TOUCH)],
            dst_ref=got[t].at[pl.ds(me_c * TOUCH, TOUCH)],
            send_sem=send_sem.at[t], recv_sem=recv_sem.at[t],
            device_id=(me_r, peer), device_id_type=MESH,
        )

    def all_parts(t):
        every = pl.ds(0, (n_col - 1) * TOUCH)
        return pltpu.make_async_remote_copy(
            src_ref=send.at[t, every], dst_ref=got[t].at[every],
            send_sem=send_sem.at[t], recv_sem=recv_sem.at[t],
            device_id=(me_r, lax.rem(me_c + 1, n_col)), device_id_type=MESH,
        )

    def pos_copy(d):
        peer = lax.rem(me_c + d, n_col)
        return pltpu.make_async_remote_copy(
            src_ref=planbuf.at[pl.ds(4, 1)], dst_ref=posbuf.at[me_c],
            send_sem=pos_send.at[d], recv_sem=pos_recv.at[d],
            device_id=(me_r, peer), device_id_type=MESH,
        )

    def posz_copy(d):
        peer = lax.rem(me_r + d, n_row)
        return pltpu.make_async_remote_copy(
            src_ref=posbuf, dst_ref=poszbuf.at[me_r],
            send_sem=posz_send.at[d], recv_sem=posz_recv.at[d],
            device_id=(peer, me_c), device_id_type=MESH,
        )

    def unit(t, row):
        if t < GROUPS:
            return comp[t].at[pl.ds(row * TOUCH, TOUCH)]
        return xbuf[t + GROUPS].at[pl.ds(row * BPD, BPD)]

    def x_copy(t, row, peer, sem):
        return pltpu.make_async_remote_copy(
            src_ref=unit(t, row), dst_ref=unit(t, row), send_sem=sem, recv_sem=xrecv_sem.at[t, row],
            device_id=(peer, me_c), device_id_type=MESH,
        )

    is_end = (me_r == 0) | (me_r == n_row - 1)

    def for_targets(t, act):
        for far in range(n_row - 1, 0, -1):
            for way, sign in enumerate((1, -1)):
                peer = me_r + sign * far
                ok = (peer >= 0) & (peer < n_row)
                if far > 1 and t >= DIRECT:
                    ok = ok & (is_end | ((peer > 0) & (peer < n_row - 1)))

                @pl.when(ok)
                def _(far=far, way=way, peer=peer):
                    act(x_copy(t, me_r, peer, xsend_sem.at[t, 2 * far + way]))

    def passed(t):
        if n_row < 4 or t < DIRECT:
            return []
        return [(1, range(2, n_row - 1), 0), (n_row - 2, range(1, n_row - 2), n_row - 1)]

    def relay(t):
        for who, rows, end in passed(t):
            @pl.when(me_r == who)
            def _(rows=rows, end=end):
                for row in rows:
                    x_copy(t, row, end, xpass_sem.at[t, row]).wait_recv()
                    x_copy(t, row, end, xpass_sem.at[t, row]).start()

    def relay_done(t):
        for who, rows, end in passed(t):
            @pl.when(me_r == who)
            def _(rows=rows, end=end):
                for row in rows:
                    x_copy(t, row, end, xpass_sem.at[t, row]).wait_send()

    def x_ready(t):
        for row in range(n_row):
            ok = me_r != row
            for who, rows, _ in passed(t):
                if row in rows:
                    ok = ok & (me_r != who)

            @pl.when(ok)
            def _(row=row):
                x_copy(t, row, lax.rem(me_r + 1, n_row), xsend_sem.at[t, 0]).wait_recv()

    def find_places():
        def block(j, carry):
            row, b = j // BPD, lax.rem(j, BPD)
            for h in range(GROUPS):
                part = pl.ds(h * width, width)
                home_q = qcol[part, :]
                place = jnp.full((width, tile), TOUCH, jnp.int32)
                for c in range(n_col):
                    place = jnp.where(home_q == c, poz[row, c, 0, me_c * BPD + b] - c * TOUCH, place)
                where[j, part, :] = place
            return carry

        lax.fori_loop(0, n_row * BPD, block, 0, unroll=2)

    def placed(h, row, b):
        place = where[row * BPD + b, pl.ds(h * width, width), :]
        value = jnp.zeros((width, tile), jnp.float32)
        for s in range(TOUCH):
            value = jnp.where(place == s, comp[h][row * TOUCH + s].astype(jnp.float32), value)
        return value

    def expand(h):
        for row in range(n_row):
            for b in range(BPD):
                xbuf[GROUPS + h][row * BPD + b] = placed(h, row, b).astype(jnp.bfloat16)

    def keep_first(h):
        for b in range(BPD):
            total[b, pl.ds(h * width, width), :] = placed(h, me_r, b)

    def reduce(t):
        k, h = divmod(t, GROUPS)
        all_parts(t).wait_recv()
        part = pl.ds(h * width, width)
        if k == 0:
            for s in range(TOUCH):
                acc = got[t][s].astype(jnp.float32)
                for c in range(1, n_col):
                    acc = acc + got[t][c * TOUCH + s].astype(jnp.float32)
                comp[t][me_r * TOUCH + s] = acc.astype(jnp.bfloat16)
        else:
            weight = coef[part, :]
            scale = weight
            for _ in range(k - 1):
                scale = scale * weight

            def block(b, carry):
                acc = got[t][poz[me_r, 0, 0, me_c * BPD + b]].astype(jnp.float32)
                for s in range(1, n_col):
                    acc = acc + got[t][poz[me_r, s, 0, me_c * BPD + b]].astype(jnp.float32)
                total[b, part, :] = total[b, part, :] + scale * acc
                if k + 1 < TERMS:
                    xbuf[t + GROUPS][me_r * BPD + b] = acc.astype(jnp.bfloat16)
                return carry

            lax.fori_loop(0, BPD, block, 0, unroll=BPD)
        if k + 1 < TERMS:
            for_targets(t, lambda copy: copy.start())

    for t in range(steps + LAG):
        if t < steps:
            if t >= GROUPS:
                if t == GROUPS:
                    for d in range(1, n_row):
                        posz_copy(d).wait_recv()
                    table = pltpu.make_async_copy(poszbuf, poz, local_sem)
                    table.start()
                    table.wait()
                    find_places()
                x_ready(t - GROUPS)
                if t < 2 * GROUPS:
                    expand(t - GROUPS)
            compute(t)
            if t == 0:
                pl.semaphore_wait(barrier, n_col - 1 + n_row - 1)
                for d in range(1, n_col):
                    pos_copy(d).start()
            for d in range(1, n_col):
                part_copy(t, d).start()
            if GROUPS <= t < 2 * GROUPS:
                keep_first(t - GROUPS)
            if t == LAG:
                for d in range(1, n_col):
                    pos_copy(d).wait_recv()
                poszbuf[me_r] = posbuf[...]
                for d in range(1, n_row):
                    posz_copy(d).start()
        if t >= LAG:
            reduce(t - LAG)
        if 0 <= t - RELAY_LAG < moves:
            relay(t - RELAY_LAG)
        old = t - 2 * LAG - 2
        if 0 <= old:
            all_parts(old).wait_send()
            if old < moves:
                for_targets(old, lambda copy: copy.wait_send())
                relay_done(old)

    for b in range(BPD):
        out_ref[pl.ds(b * tile, tile), :] = jnp.transpose(total[b])
    for d in range(1, n_col):
        pos_copy(d).wait_send()
    for d in range(1, n_row):
        posz_copy(d).wait_send()
    for t in range(steps + LAG - 2 * LAG - 2, steps):
        all_parts(t).wait_send()


def shards(tiles, tile_row, tile_col, tile_count, query_ids, damping):
    tile_block = tiles[0, 0]
    slots, tile, _ = tile_block.shape
    queries = query_ids.shape[0]
    n_row = lax.axis_size("row")
    n_col = lax.axis_size("col")
    width = queries // GROUPS
    steps = TERMS * GROUPS
    moves = steps - GROUPS
    bf16 = jnp.bfloat16
    dma = pltpu.SemaphoreType.DMA
    smem = pl.BlockSpec(memory_space=pltpu.SMEM)
    vmem = pl.BlockSpec(memory_space=pltpu.VMEM)
    return pl.pallas_call(
        functools.partial(katz_kernel, n_row, n_col),
        out_shape=jax.ShapeDtypeStruct((BPD * tile, queries), jnp.float32),
        in_specs=[smem] + [vmem] * 4 + [pl.BlockSpec(memory_space=pl.ANY)],
        out_specs=vmem,
        scratch_shapes=[
            pltpu.VMEM((slots, tile, tile), bf16),
            pltpu.VMEM((slots, tile, tile), bf16),
            pltpu.VMEM((slots, width, tile), bf16),
            pltpu.VMEM((steps, n_col * TOUCH, width, tile), bf16),
            [pltpu.VMEM((n_col * TOUCH + 1, width, tile), bf16)] * steps,
            [pltpu.VMEM((n_row * BPD, width, tile), bf16)] * steps,
            [pltpu.VMEM((n_row * TOUCH, width, tile), bf16)] * GROUPS,
            pltpu.VMEM((BPD, queries, tile), jnp.float32),
            pltpu.VMEM((queries, tile), jnp.float32),
            pltpu.VMEM((queries, tile), jnp.int32),
            pltpu.VMEM((8, slots), jnp.int32),
            pltpu.VMEM((n_col, 1, slots), jnp.int32),
            pltpu.VMEM((n_row, n_col, 1, slots), jnp.int32),
            pltpu.VMEM((n_row * BPD, queries, tile), jnp.int32),
            pltpu.SMEM((8, slots), jnp.int32),
            pltpu.SMEM((n_row, n_col, 1, slots), jnp.int32),
            dma((CHUNKS,)), dma((n_col,)), dma((n_col,)), dma((n_row,)), dma((n_row,)), dma,
            dma((steps,)), dma((steps,)),
            dma((moves, 2 * n_row)), dma((moves, n_row)), dma((moves, n_row)),
        ],
        compiler_params=pltpu.CompilerParams(
            collective_id=0, has_side_effects=True, vmem_limit_bytes=60 * 1024 * 1024
        ),
    )(
        tile_count[:1, :1], tile_row[0], tile_col[0],
        query_ids.reshape(1, queries), damping.reshape(1, queries), tile_block,
    )


def solution(mesh):
    in_specs = (
        P("row", "col", None, None, None),
        P("row", "col", None),
        P("row", "col", None),
        P("row", "col"),
        P(),
        P(),
    )
    out_specs = P(("row", "col"), None)
    return jax.shard_map(shards, mesh=mesh, in_specs=in_specs, out_specs=out_specs, check_vma=False)
```

```python
import functools

import jax
import jax.numpy as jnp
from jax import lax
from jax.experimental import pallas as pl
from jax.experimental.pallas import tpu as pltpu
from jax.sharding import PartitionSpec as P

BPD = 8
TERMS = 4
TOUCH = 4
GROUPS = 8
UNROLL = 128
CHUNKS = 8
LAG = 2
RELAY_LAG = 4
MESH = pl.DeviceIdType.MESH


def plan(rows, cols, count, n_col, me_col):
    slots = rows.shape[1]
    row_blocks = BPD * n_col
    square = (slots, slots)
    lane = lax.broadcasted_iota(jnp.int32, square, 1)
    sub = lax.broadcasted_iota(jnp.int32, square, 0)

    def across(row):
        return jnp.broadcast_to(row, square)

    def down(row):
        return jnp.transpose(jnp.broadcast_to(row, square))

    def total(mask, value=1):
        return jnp.sum(jnp.where(mask, value, 0), axis=0, keepdims=True)

    key = jnp.where(lane[:1] < count, rows, row_blocks)
    key_l, key_s = across(key), down(key)
    twin = (key_s == key_l) & (sub < lane)
    rank = total((key_s < key_l) | twin)
    again = jnp.minimum(total(twin), 1)
    packed = lane[:1] + slots * (again + 2 * cols)
    ordered = total(down(rank) == lane, down(packed))
    perm = lax.rem(ordered, slots)
    rest = lax.div(ordered, slots)
    cont = lax.rem(rest, 2)
    scol = lax.div(rest, 2)

    marked = jnp.minimum(total(key_s == lane), 1)
    marked = jnp.where(lane[:1] < row_blocks, marked, 0)
    last = total(key_s <= lane) - 1
    owner_l = lax.div(lane[:1], BPD)
    first = owner_l * BPD
    place = total((sub >= across(first)) & (sub < lane), down(marked))
    slot_of = jnp.where(marked > 0, owner_l * TOUCH + place, -1)
    ends = total(down(slot_of) == lane, down(last))
    pos = jnp.where(marked > 0, me_col * TOUCH + place, n_col * TOUCH)
    return perm, scol, cont, ends, pos


def katz_kernel(
    n_row, n_col,
    count_ref, rows_ref, cols_ref, qid_ref, damp_ref, tiles_hbm,
    out_ref,
    tiles, flip, run, send, got, xbuf, comp, total, coef, qcol, planbuf, posbuf, poszbuf, where, order, poz,
    tile_sem, pos_send, pos_recv, posz_send, posz_recv, local_sem, send_sem, recv_sem, xsend_sem, xrecv_sem,
):
    me_r = lax.axis_index("row")
    me_c = lax.axis_index("col")
    slots, tile, _ = tiles.shape
    queries = qid_ref.shape[1]
    width = queries // GROUPS
    steps = TERMS * GROUPS
    moves = steps - GROUPS
    piece = slots // CHUNKS

    def load(i):
        part = pl.ds(i * piece, piece)
        return pltpu.make_async_copy(tiles_hbm.at[part], tiles.at[part], tile_sem.at[i])

    for i in range(CHUNKS):
        load(i).start()
    barrier = pltpu.get_barrier_semaphore()
    for d in range(1, n_col):
        pl.semaphore_signal(barrier, inc=1, device_id=(me_r, lax.rem(me_c + d, n_col)), device_id_type=MESH)
    for d in range(1, n_row):
        pl.semaphore_signal(barrier, inc=1, device_id=(lax.rem(me_r + d, n_row), me_c), device_id_type=MESH)

    perm, scol, cont, ends, pos = plan(rows_ref[...], cols_ref[...], count_ref[0, 0], n_col, me_c)
    planbuf[0:1, :] = perm
    planbuf[1:2, :] = scol
    planbuf[2:3, :] = cont
    planbuf[3:4, :] = ends
    planbuf[4:5, :] = pos
    posbuf[me_c] = pos
    spill = pltpu.make_async_copy(planbuf, order, local_sem)
    spill.start()

    lane = lax.broadcasted_iota(jnp.int32, (queries, tile), 1)
    ids = qid_ref[...]
    qid = jnp.transpose(jnp.broadcast_to(ids, (tile, queries))) - lane
    coef[...] = jnp.transpose(jnp.broadcast_to(damp_ref[...], (tile, queries)))
    home = lax.rem(lax.div(ids, BPD * tile), n_col)
    qcol[...] = jnp.transpose(jnp.broadcast_to(home, (tile, queries)))

    def first_x(j, carry):
        base = ((j // BPD * n_col + me_c) * BPD + lax.rem(j, BPD)) * tile
        hot = jnp.where(qid == base, 1.0, 0.0).astype(jnp.bfloat16)
        for h in range(GROUPS):
            xbuf[h][j] = hot[h * width:(h + 1) * width]
        return carry

    lax.fori_loop(0, n_row * BPD, first_x, 0)
    for t in range(GROUPS, steps):
        got[t][n_col * TOUCH] = jnp.zeros((width, tile), jnp.bfloat16)
    for i in range(CHUNKS):
        load(i).wait()

        def turn(s, carry):
            flip[s] = jnp.transpose(tiles[s])
            return carry

        lax.fori_loop(i * piece, (i + 1) * piece, turn, 0, unroll=8)
    spill.wait()

    def compute(t):
        both = 2 * width

        def body(i, acc):
            for u in range(0, UNROLL, 2):
                p = i * UNROLL + u
                weights = jnp.concatenate([flip[order[0, p]], flip[order[0, p + 1]]], axis=1)
                left, right = order[1, p], order[1, p + 1]
                x = jnp.concatenate([xbuf[t][left], xbuf[t + 1][left], xbuf[t][right], xbuf[t + 1][right]], axis=0)
                prod = jnp.dot(x, weights, preferred_element_type=jnp.float32)
                acc = jnp.where(order[2, p] > 0, acc, 0.0) + prod[:both, :tile]
                run[p] = acc.astype(jnp.bfloat16)
                acc = jnp.where(order[2, p + 1] > 0, acc, 0.0) + prod[both:, tile:]
                run[p + 1] = acc.astype(jnp.bfloat16)
            return acc

        lax.fori_loop(0, slots // UNROLL, body, jnp.zeros((both, tile), jnp.float32))
        for s in range(n_col * TOUCH):
            value = run[order[3, s]]
            send[t, s] = value[:width]
            send[t + 1, s] = value[width:]
        for j in range(TOUCH):
            value = run[order[3, me_c * TOUCH + j]]
            got[t][me_c * TOUCH + j] = value[:width]
            got[t + 1][me_c * TOUCH + j] = value[width:]

    def part_copy(t, d):
        peer = lax.rem(me_c + d, n_col)
        return pltpu.make_async_remote_copy(
            src_ref=send.at[t, pl.ds(peer * TOUCH, TOUCH)],
            dst_ref=got[t].at[pl.ds(me_c * TOUCH, TOUCH)],
            send_sem=send_sem, recv_sem=recv_sem.at[t],
            device_id=(me_r, peer), device_id_type=MESH,
        )

    def all_parts(t):
        every = pl.ds(0, (n_col - 1) * TOUCH)
        return pltpu.make_async_remote_copy(
            src_ref=send.at[t, every], dst_ref=got[t].at[every],
            send_sem=send_sem, recv_sem=recv_sem.at[t],
            device_id=(me_r, lax.rem(me_c + 1, n_col)), device_id_type=MESH,
        )

    def pos_copy(d):
        peer = lax.rem(me_c + d, n_col)
        return pltpu.make_async_remote_copy(
            src_ref=planbuf.at[pl.ds(4, 1)], dst_ref=posbuf.at[me_c],
            send_sem=pos_send.at[d], recv_sem=pos_recv.at[d],
            device_id=(me_r, peer), device_id_type=MESH,
        )

    def posz_copy(d):
        peer = lax.rem(me_r + d, n_row)
        return pltpu.make_async_remote_copy(
            src_ref=posbuf, dst_ref=poszbuf.at[me_r],
            send_sem=posz_send.at[d], recv_sem=posz_recv.at[d],
            device_id=(peer, me_c), device_id_type=MESH,
        )

    def unit(t, row):
        if t < GROUPS:
            return comp[t].at[pl.ds(row * TOUCH, TOUCH)]
        return xbuf[t + GROUPS].at[pl.ds(row * BPD, BPD)]

    def relays(t):
        if n_row < 4 or t < GROUPS:
            return []
        return [(1, 2, 0), (n_row - 2, 1, n_row - 1)]

    def x_copy(t, first, rows, peer, sem, kind):
        size = TOUCH if t < GROUPS else BPD
        part = (comp[t] if t < GROUPS else xbuf[t + GROUPS]).at[pl.ds(first * size, rows * size)]
        return pltpu.make_async_remote_copy(
            src_ref=part, dst_ref=part, send_sem=sem, recv_sem=xrecv_sem.at[t, kind],
            device_id=(peer, me_c), device_id_type=MESH,
        )

    is_end = (me_r == 0) | (me_r == n_row - 1)
    is_relay = (me_r == 1) | (me_r == n_row - 2)

    def send_x(t):
        for d in range(n_row - 1, 0, -1):
            peer = lax.rem(me_r + jnp.where(2 * me_r < n_row, d, n_row - d), n_row)
            if not relays(t):
                x_copy(t, me_r, 1, peer, xsend_sem.at[0], 0).start()
            else:
                far = jnp.abs(peer - me_r) > 1
                onward = ((peer == 1) & (me_r > 1)) | ((peer == n_row - 2) & (me_r < n_row - 2))
                kind = jnp.where(onward & jnp.logical_not(is_end), 1, 0)

                @pl.when(is_end | jnp.logical_not(far & ((peer == 0) | (peer == n_row - 1))))
                def _(peer=peer, kind=kind):
                    x_copy(t, me_r, 1, peer, xsend_sem.at[1], kind).start()

    def relay(t):
        for who, first, end in relays(t):
            @pl.when(me_r == who)
            def _(first=first, end=end):
                x_copy(t, first, n_row - 3, end, xsend_sem.at[2], 1).wait_recv()
                x_copy(t, first, n_row - 3, end, xsend_sem.at[2], 0).start()

    def x_ready(t):
        peer = lax.rem(me_r + 1, n_row)
        if not relays(t):
            x_copy(t, 0, n_row - 1, peer, xsend_sem.at[0], 0).wait_recv()
        else:
            @pl.when(is_relay)
            def _():
                x_copy(t, 0, 2, peer, xsend_sem.at[1], 0).wait_recv()

            @pl.when(jnp.logical_not(is_relay))
            def _():
                x_copy(t, 0, n_row - 1, peer, xsend_sem.at[1], 0).wait_recv()

    def sent(rows, sem):
        size = rows * width * tile
        whole, rest = divmod(size, tile * tile)
        assert rest == 0 and whole <= slots
        part = tiles.at[pl.ds(0, whole)]
        pltpu.make_async_remote_copy(
            src_ref=part, dst_ref=part, send_sem=sem, recv_sem=xrecv_sem.at[0, 0],
            device_id=(lax.rem(me_r + 1, n_row), me_c), device_id_type=MESH,
        ).wait_send()

    def all_x_sent():
        sent(GROUPS * (n_row - 1) * TOUCH, xsend_sem.at[0])
        later = (moves - GROUPS) * BPD
        if n_row < 4:
            sent(later * (n_row - 1), xsend_sem.at[1])
            return

        @pl.when(is_end)
        def _():
            sent(later * (n_row - 1), xsend_sem.at[1])

        @pl.when(is_relay)
        def _():
            sent(later * (n_row - 2), xsend_sem.at[1])
            sent(later * (n_row - 3), xsend_sem.at[2])

        if n_row > 4:
            @pl.when(jnp.logical_not(is_end | is_relay))
            def _():
                sent(later * (n_row - 3), xsend_sem.at[1])

    def find_places():
        sub = lax.broadcasted_iota(jnp.int32, (n_col, tile), 0)
        lane_c = lax.broadcasted_iota(jnp.int32, (queries, n_col), 1)
        is_home = jnp.where(qcol[:, :n_col] == lane_c, 1.0, 0.0).astype(jnp.bfloat16)

        def block(j, carry):
            row, b = j // BPD, lax.rem(j, BPD)
            table = jnp.zeros((n_col, tile), jnp.int32)
            for c in range(n_col):
                table = jnp.where(sub == c, poz[row, c, 0, me_c * BPD + b] - c * TOUCH, table)
            table = jnp.minimum(table, TOUCH).astype(jnp.float32).astype(jnp.bfloat16)
            where[j] = jnp.dot(is_home, table, preferred_element_type=jnp.float32)
            return carry

        lax.fori_loop(0, n_row * BPD, block, 0, unroll=BPD)

    def placed(h, row, b):
        place = where[row * BPD + b, pl.ds(h * width, width), :]
        value = jnp.zeros((width, tile), jnp.float32)
        for s in range(TOUCH):
            value = jnp.where(place == float(s), comp[h][row * TOUCH + s].astype(jnp.float32), value)
        return value

    def expand(h):
        for row in range(n_row):
            for b in range(BPD):
                xbuf[GROUPS + h][row * BPD + b] = placed(h, row, b).astype(jnp.bfloat16)

    def keep_first(h):
        for b in range(BPD):
            total[b, pl.ds(h * width, width), :] = placed(h, me_r, b)

    def reduce(t):
        k, h = divmod(t, GROUPS)
        all_parts(t).wait_recv()
        part = pl.ds(h * width, width)
        if k == 0:
            for s in range(TOUCH):
                acc = got[t][s].astype(jnp.float32)
                for c in range(1, n_col):
                    acc = acc + got[t][c * TOUCH + s].astype(jnp.float32)
                comp[t][me_r * TOUCH + s] = acc.astype(jnp.bfloat16)
        else:
            weight = coef[part, :]
            scale = weight
            for _ in range(k - 1):
                scale = scale * weight

            def block(b, carry):
                acc = got[t][poz[me_r, 0, 0, me_c * BPD + b]].astype(jnp.float32)
                for s in range(1, n_col):
                    acc = acc + got[t][poz[me_r, s, 0, me_c * BPD + b]].astype(jnp.float32)
                total[b, part, :] = total[b, part, :] + scale * acc
                if k + 1 < TERMS:
                    xbuf[t + GROUPS][me_r * BPD + b] = acc.astype(jnp.bfloat16)
                return carry

            lax.fori_loop(0, BPD, block, 0, unroll=BPD)
        if k + 1 < TERMS:
            send_x(t)

    for t in range(0, steps + LAG + 1, 2):
        if t < steps:
            if t >= GROUPS:
                for h in (t - GROUPS, t - GROUPS + 1):
                    x_ready(h)
                    if h < GROUPS:
                        expand(h)
            compute(t)
            if t == 0:
                pl.semaphore_wait(barrier, n_col - 1 + n_row - 1)
                for d in range(1, n_col):
                    pos_copy(d).start()
            for h in (t, t + 1):
                for d in range(1, n_col):
                    part_copy(h, d).start()
            if t == 2:
                for d in range(1, n_col):
                    pos_copy(d).wait_recv()
                poszbuf[me_r] = posbuf[...]
                for d in range(1, n_row):
                    posz_copy(d).start()
            if t == GROUPS - 2:
                for d in range(1, n_row):
                    posz_copy(d).wait_recv()
                table = pltpu.make_async_copy(poszbuf, poz, local_sem)
                table.start()
                table.wait()
                find_places()
            if GROUPS <= t < 2 * GROUPS:
                keep_first(t - GROUPS)
                keep_first(t - GROUPS + 1)
        for j in (t, t + 1):
            if 0 <= j - LAG < steps:
                reduce(j - LAG)
            if 0 <= j - RELAY_LAG < moves:
                relay(j - RELAY_LAG)

    for b in range(BPD):
        out_ref[pl.ds(b * tile, tile), :] = jnp.transpose(total[b])
    for d in range(1, n_col):
        pos_copy(d).wait_send()
    for d in range(1, n_row):
        posz_copy(d).wait_send()
    every = send.at[:, pl.ds(0, (n_col - 1) * TOUCH)]
    pltpu.make_async_remote_copy(
        src_ref=every, dst_ref=every, send_sem=send_sem, recv_sem=recv_sem.at[0],
        device_id=(me_r, lax.rem(me_c + 1, n_col)), device_id_type=MESH,
    ).wait_send()
    all_x_sent()


def shards(tiles, tile_row, tile_col, tile_count, query_ids, damping):
    tile_block = tiles[0, 0]
    slots, tile, _ = tile_block.shape
    queries = query_ids.shape[0]
    n_row = lax.axis_size("row")
    n_col = lax.axis_size("col")
    width = queries // GROUPS
    steps = TERMS * GROUPS
    moves = steps - GROUPS
    bf16 = jnp.bfloat16
    dma = pltpu.SemaphoreType.DMA
    smem = pl.BlockSpec(memory_space=pltpu.SMEM)
    vmem = pl.BlockSpec(memory_space=pltpu.VMEM)
    return pl.pallas_call(
        functools.partial(katz_kernel, n_row, n_col),
        out_shape=jax.ShapeDtypeStruct((BPD * tile, queries), jnp.float32),
        in_specs=[smem] + [vmem] * 4 + [pl.BlockSpec(memory_space=pl.ANY)],
        out_specs=vmem,
        scratch_shapes=[
            pltpu.VMEM((slots, tile, tile), bf16),
            pltpu.VMEM((slots, tile, tile), bf16),
            pltpu.VMEM((slots, 2 * width, tile), bf16),
            pltpu.VMEM((steps, n_col * TOUCH, width, tile), bf16),
            [pltpu.VMEM((n_col * TOUCH + 1, width, tile), bf16)] * steps,
            [pltpu.VMEM((n_row * BPD, width, tile), bf16)] * steps,
            [pltpu.VMEM((n_row * TOUCH, width, tile), bf16)] * GROUPS,
            pltpu.VMEM((BPD, queries, tile), jnp.float32),
            pltpu.VMEM((queries, tile), jnp.float32),
            pltpu.VMEM((queries, tile), jnp.int32),
            pltpu.VMEM((8, slots), jnp.int32),
            pltpu.VMEM((n_col, 1, slots), jnp.int32),
            pltpu.VMEM((n_row, n_col, 1, slots), jnp.int32),
            pltpu.VMEM((n_row * BPD, queries, tile), jnp.float32),
            pltpu.SMEM((8, slots), jnp.int32),
            pltpu.SMEM((n_row, n_col, 1, slots), jnp.int32),
            dma((CHUNKS,)), dma((n_col,)), dma((n_col,)), dma((n_row,)), dma((n_row,)), dma,
            dma, dma((steps,)),
            dma((3,)), dma((moves, 2)),
        ],
        compiler_params=pltpu.CompilerParams(
            collective_id=0, has_side_effects=True, vmem_limit_bytes=60 * 1024 * 1024
        ),
    )(
        tile_count[:1, :1], tile_row[0], tile_col[0],
        query_ids.reshape(1, queries), damping.reshape(1, queries), tile_block,
    )


def solution(mesh):
    in_specs = (
        P("row", "col", None, None, None),
        P("row", "col", None),
        P("row", "col", None),
        P("row", "col"),
        P(),
        P(),
    )
    out_specs = P(("row", "col"), None)
    return jax.shard_map(shards, mesh=mesh, in_specs=in_specs, out_specs=out_specs, check_vma=False)
```
